32 devices in a mesh: rows: 8 (over z, x), cols: 4 (over y, core).
Axes of the slice: x: 2, y: 2, z: 4, core: 2. Of those that a mesh axis runs over, the one named last changes fastest.
Arguments:
- margins: bfloat16 [8192, 2048], P(('rows', 'cols')), may hold values from -512 to 512
- subset_masks: bfloat16 [8192, 8192], P('rows'), may hold values from 0 to 1
- ridge_param: float32 [], replicated, may hold values from 1024 to 4096
Outputs:
- weights: float32 [8192, 2048], P('rows', 'cols')
- residual_norm: float32 [2048], P('cols')
The draws below stay inside these ranges and needn't reach their ends.
All inputs are finite; a program needn't handle non-finite values.
Results may differ from the reference program's by a relative error of at most 0.0021.
Values may be sent and summed in bfloat16 or wider, within the bound.
No kernel may reach another device: no remote copies, remote signals or barrier semaphores. Data moves between devices by JAX's collectives and lax.ppermute only.
A program may use at most 128 MiB of HBM per device.

```python
import math
import jax
import jax.numpy as jnp
from jax import lax

N = 8192
E = 2048
ITERS = 2
M = 8192


def draw_subset_masks(key, part):
    uniform = jax.random.uniform(key, (M, N), jnp.float32)
    return (uniform < 0.5).astype(jnp.float32).astype(jnp.bfloat16)


def block_scale(rng, extent, pieces, smallest, high):
    level, own = 1.0, jax.random.fold_in(rng, 6)
    for position, shards_of in pieces:
        steps = jnp.exp(jax.random.uniform(jax.random.fold_in(own, position), (shards_of,), jnp.float32, smallest / len(pieces), high / len(pieces)))
        level = level * jnp.repeat(steps, extent[position] // shards_of).reshape([-1 if axis == position else 1 for axis in range(len(extent))])
    return level


def normal_values(key, dims, deviation, reach, split=(), dtype=jnp.bfloat16):
    result = jax.random.normal(key, dims, jnp.float32) * deviation
    if len(split) > 0:
        result = block_scale(key, dims, split, -0.22, 0.18) * result
    return jnp.clip(result, min=-reach, max=reach).astype(dtype)


def setup_inputs(seed: int = 0) -> dict:
    arg_keys = jax.random.split(jax.random.key(seed), 4)
    margins = normal_values(arg_keys[0], (M, E), 64.0, 512.0, ((0, 32),))
    subset_masks = draw_subset_masks(jax.random.fold_in(arg_keys[3], 71), 0)
    ridge_param = jnp.clip(jnp.exp(jax.random.uniform(arg_keys[2], (), jnp.float32, math.log(1024.0), math.log(4096.0))), 1024.0, 4096.0)
    return dict(margins=margins, subset_masks=subset_masks, ridge_param=ridge_param)


def rounded(values):
    low = lax.optimization_barrier(values.astype(jnp.bfloat16))
    return low.astype(jnp.float32)

def reference(margins, subset_masks, ridge_param):
    design = 2.0 * subset_masks.astype(jnp.float32) - 1.0
    highest = lax.Precision.HIGHEST
    target = jnp.dot(design.T, margins.astype(jnp.float32), precision=highest)
    first_norms = lax.optimization_barrier(jnp.sum(target * target, axis=0))
    weights = jnp.zeros_like(target)
    residual = target
    direction = target
    norm_now = first_norms
    for iteration in range(ITERS):
        dir_low = rounded(direction)
        fitted = jnp.dot(design, dir_low, precision=highest)
        fitted_low = rounded(fitted)
        image = jnp.dot(design.T, fitted_low, precision=highest) + ridge_param * direction
        curvature = lax.optimization_barrier(jnp.sum(dir_low * image, axis=0))
        alpha = norm_now / curvature
        weights = weights + alpha * direction
        residual = residual - alpha * image
        norm_next = lax.optimization_barrier(jnp.sum(residual * residual, axis=0))
        direction = residual + norm_next / norm_now * direction
        norm_now = norm_next
    return (weights, jnp.sqrt(norm_now / first_norms))
```

```python
import jax
import jax.numpy as jnp
from jax import lax
from jax.sharding import PartitionSpec as P


GROUPS = 2
CHAINS = 2
HEADROOM = 32768.0


def ring_block(position, size):
    return jnp.where(position < size // 2, 2 * position, 2 * (size - 1 - position) + 1)


def ring_position(block, size):
    return jnp.where(block % 2 == 0, block // 2, size - 1 - block // 2)


def ring_order(size):
    return [2 * q if q < size // 2 else 2 * (size - 1 - q) + 1 for q in range(size)]


def make_body(rows_size, cols_size):
    order = ring_order(rows_size)
    up = [(order[q], order[(q + 1) % rows_size]) for q in range(rows_size)]
    down = [(b, a) for a, b in up]
    perms = (up, down)

    def total(x, axis, size):
        step = 1
        while step < size:
            x = x + lax.ppermute(x, axis, [(i, i ^ step) for i in range(size)])
            step *= 2
        return x

    def per_device(margins, subset_masks, ridge_param):
        local_subsets, n = subset_masks.shape
        piece, e = margins.shape
        subsets = local_subsets * rows_size
        columns = e // cols_size
        width = columns // GROUPS
        block = n // rows_size
        chain = block // CHAINS
        me = lax.axis_index("rows")
        position = ring_position(me, rows_size)
        mycol = lax.axis_index("cols")
        groups = range(GROUPS)
        blocks = [ring_block((position + j) % rows_size, rows_size) for j in range(rows_size)]

        sizes = jnp.sum(jnp.abs(margins.astype(jnp.float32)), axis=0, keepdims=True)
        l1 = None
        for step in range(cols_size):
            sent = lax.dynamic_slice(sizes, (0, (mycol ^ step) * columns), (1, columns))
            if step:
                sent = lax.ppermute(sent, "cols", [(i, i ^ step) for i in range(cols_size)])
            l1 = sent if l1 is None else l1 + sent
        target_bound = jnp.maximum(total(l1, "rows", rows_size) * 1.01, 1e-30)

        regrouped = jnp.zeros((local_subsets, columns), margins.dtype)
        for step in range(cols_size):
            other = mycol ^ step
            sent = lax.dynamic_slice(margins, (0, other * columns), (piece, columns))
            if step:
                sent = lax.ppermute(sent, "cols", [(i, i ^ step) for i in range(cols_size)])
            regrouped = lax.dynamic_update_slice(regrouped, sent, (other * piece, 0))

        design = lax.optimization_barrier(subset_masks * 2 - 1)

        def design_rows(b, c, early=False):
            at = (0, b * block + c * chain)
            if early:
                return lax.dynamic_slice(subset_masks, at, (local_subsets, chain)) * 2 - 1
            return lax.dynamic_slice(design, at, (local_subsets, chain))

        def group_of(x, g):
            return x[:, g * width : (g + 1) * width]

        def scatter_sums(operands, bounds, early=0):
            scale = [HEADROOM / b for b in bounds]
            inverse = [b * (1.0 / HEADROOM) for b in bounds]

            def partial(g, c, s, b):
                return lax.dot_general(
                    design_rows(b, c, s < early), operands[g], (((0,), (0,)), ((), ())),
                    preferred_element_type=jnp.float32,
                )

            keys = [(g, c) for c in range(CHAINS) for g in range(GROUPS)]
            held = {}
            for s in range(rows_size):
                for g, c in keys:
                    j = (rows_size - 1 - s) if g == 0 else (s + 1) % rows_size
                    value = partial(g, c, s, blocks[j])
                    scale[g], inverse[g] = lax.optimization_barrier((scale[g], inverse[g]))
                    if s:
                        value = value + held[g, c].astype(jnp.float32) * inverse[g]
                    if s < rows_size - 1:
                        value = (value * scale[g]).astype(jnp.float16)
                        value = lax.ppermute(value, "rows", perms[g])
                    held[g, c] = value
            return [jnp.concatenate([held[g, c] for c in range(CHAINS)], axis=0) for g in range(GROUPS)]

        def gather_times(lows):
            keys = [(g, c) for c in range(CHAINS) for g in range(GROUPS)]
            held = {(g, c): lows[g][c * chain : (c + 1) * chain] for g, c in keys}
            result = [None] * GROUPS
            for s in range(rows_size):
                following = {}
                for g, c in keys:
                    if s < rows_size - 1:
                        following[g, c] = lax.ppermute(held[g, c], "rows", perms[g])
                for g, c in keys:
                    j = (rows_size - s) % rows_size if g == 0 else s
                    product = jnp.dot(
                        design_rows(blocks[j], c), held[g, c], preferred_element_type=jnp.float32
                    )
                    result[g] = product if result[g] is None else result[g] + product
                held = following
            return result

        def column_sum(x):
            return jnp.sum(x, axis=0, keepdims=True)

        target = scatter_sums(
            [group_of(regrouped, g) for g in groups], [group_of(target_bound, g) for g in groups],
            early=2,
        )
        first_norms = [total(column_sum(t * t), "rows", rows_size) for t in target]
        lows = [t.astype(jnp.bfloat16) for t in target]
        fitted0 = gather_times(lows)
        fitted_low = [f.astype(jnp.bfloat16) for f in fitted0]
        curvature = [
            total(
                column_sum(fitted0[g] * fitted_low[g].astype(jnp.float32))
                + ridge_param * column_sum(lows[g].astype(jnp.float32) * target[g]),
                "rows", rows_size,
            )
            for g in groups
        ]
        gain = 1.02 * subsets * float(n) ** 0.5
        image = scatter_sums(
            fitted_low, [jnp.maximum(gain * jnp.sqrt(v), 1e-30) for v in first_norms]
        )
        alpha0 = [first_norms[g] / curvature[g] for g in groups]
        residual = [
            target[g] - alpha0[g] * (image[g] + ridge_param * target[g]) for g in groups
        ]
        norm1 = [total(column_sum(r * r), "rows", rows_size) for r in residual]
        beta = [norm1[g] / first_norms[g] for g in groups]
        direction = [residual[g] + beta[g] * target[g] for g in groups]
        fresh = gather_times([r.astype(jnp.bfloat16) for r in residual])
        fitted1 = [fresh[g] + beta[g] * fitted0[g] for g in groups]
        fitted_low = [f.astype(jnp.bfloat16) for f in fitted1]
        curvature = [
            total(
                column_sum(fitted1[g] * fitted_low[g].astype(jnp.float32))
                + ridge_param * column_sum(direction[g] * direction[g]),
                "rows", rows_size,
            )
            for g in groups
        ]
        direction_norm = [norm1[g] + beta[g] * beta[g] * first_norms[g] for g in groups]
        image = scatter_sums(
            fitted_low, [jnp.maximum(1.5 * gain * jnp.sqrt(v), 1e-30) for v in direction_norm]
        )
        alpha1 = [norm1[g] / curvature[g] for g in groups]
        weights = jnp.concatenate(
            [alpha0[g] * target[g] + alpha1[g] * direction[g] for g in groups], axis=1
        )
        residual = [
            residual[g] - alpha1[g] * (image[g] + ridge_param * direction[g]) for g in groups
        ]
        last = jnp.concatenate([column_sum(r * r) for r in residual], axis=1)
        last = total(last, "rows", rows_size)
        ratio = last / jnp.concatenate(first_norms, axis=1)
        return weights, jnp.sqrt(ratio).reshape(columns)

    return per_device


def solution(mesh):
    in_specs = (P(("rows", "cols"), None), P("rows", None), P())
    out_specs = (P("rows", "cols"), P("cols"))
    body = make_body(mesh.shape["rows"], mesh.shape["cols"])

    return jax.shard_map(body, mesh=mesh, in_specs=in_specs, out_specs=out_specs, check_vma=False)
```

```python
import jax
import jax.numpy as jnp
from jax import lax
from jax.sharding import PartitionSpec as P


GROUPS = 2
CHAINS = 2
HEADROOM = 32768.0


def ring_block(position, size):
    return jnp.where(position < size // 2, 2 * position, 2 * (size - 1 - position) + 1)


def ring_position(block, size):
    return jnp.where(block % 2 == 0, block // 2, size - 1 - block // 2)


def ring_order(size):
    return [2 * q if q < size // 2 else 2 * (size - 1 - q) + 1 for q in range(size)]


def stages(size):
    return size.bit_length() - 1


def make_body(rows_size, cols_size):
    order = ring_order(rows_size)
    up = [(order[q], order[(q + 1) % rows_size]) for q in range(rows_size)]
    down = [(b, a) for a, b in up]
    perms = (up, down)

    def total(x):
        for stage in range(stages(rows_size)):
            sent = lax.ppermute(x, "rows", [(i, i ^ (1 << stage)) for i in range(rows_size)])
            x = x + sent
        return x

    def per_device(margins, subset_masks, ridge_param):
        local_subsets, n = subset_masks.shape
        piece, e = margins.shape
        subsets = local_subsets * rows_size
        columns = e // cols_size
        width = columns // GROUPS
        block = n // rows_size
        chain = block // CHAINS
        me = lax.axis_index("rows")
        position = ring_position(me, rows_size)
        mycol = lax.axis_index("cols")
        groups = range(GROUPS)
        blocks = [ring_block((position + j) % rows_size, rows_size) for j in range(rows_size)]

        sizes = jnp.sum(jnp.abs(margins.astype(jnp.float32)), axis=0, keepdims=True)
        l1 = None
        for step in range(cols_size):
            sent = lax.dynamic_slice(sizes, (0, (mycol ^ step) * columns), (1, columns))
            if step:
                sent = lax.ppermute(sent, "cols", [(i, i ^ step) for i in range(cols_size)])
            l1 = sent if l1 is None else l1 + sent
        target_bound = jnp.maximum(total(l1) * 1.01, 1e-30)

        regrouped = jnp.zeros((local_subsets, columns), margins.dtype)
        for step in range(cols_size):
            other = mycol ^ step
            sent = lax.dynamic_slice(margins, (0, other * columns), (piece, columns))
            if step:
                sent = lax.ppermute(sent, "cols", [(i, i ^ step) for i in range(cols_size)])
            regrouped = lax.dynamic_update_slice(regrouped, sent, (other * piece, 0))

        design = lax.optimization_barrier(subset_masks * 2 - 1)

        def design_rows(b, c, early=False):
            at = (0, b * block + c * chain)
            if early:
                return lax.dynamic_slice(subset_masks, at, (local_subsets, chain)) * 2 - 1
            return lax.dynamic_slice(design, at, (local_subsets, chain))

        def group_of(x, g):
            return x[:, g * width : (g + 1) * width]

        def scatter_sums(operands, bounds, early=0):
            scale = [HEADROOM / b for b in bounds]
            inverse = [b * (1.0 / HEADROOM) for b in bounds]

            def partial(g, c, s, b):
                return lax.dot_general(
                    design_rows(b, c, s < early), operands[g], (((0,), (0,)), ((), ())),
                    preferred_element_type=jnp.float32,
                )

            keys = [(g, c) for c in range(CHAINS) for g in range(GROUPS)]
            held = {}
            for s in range(rows_size):
                for g, c in keys:
                    j = (rows_size - 1 - s) if g == 0 else (s + 1) % rows_size
                    value = partial(g, c, s, blocks[j])
                    scale[g], inverse[g] = lax.optimization_barrier((scale[g], inverse[g]))
                    if s:
                        value = value + held[g, c].astype(jnp.float32) * inverse[g]
                    if s < rows_size - 1:
                        value = (value * scale[g]).astype(jnp.float16)
                        value = lax.ppermute(value, "rows", perms[g])
                    held[g, c] = value
            return [jnp.concatenate([held[g, c] for c in range(CHAINS)], axis=0) for g in range(GROUPS)]

        def gather_times(lows):
            keys = [(g, c) for c in range(CHAINS) for g in range(GROUPS)]
            held = {(g, c): lows[g][c * chain : (c + 1) * chain] for g, c in keys}
            result = [None] * GROUPS
            for s in range(rows_size):
                following = {}
                for g, c in keys:
                    if s < rows_size - 1:
                        following[g, c] = lax.ppermute(held[g, c], "rows", perms[g])
                for g, c in keys:
                    j = (rows_size - s) % rows_size if g == 0 else s
                    product = jnp.dot(
                        design_rows(blocks[j], c), held[g, c], preferred_element_type=jnp.float32
                    )
                    result[g] = product if result[g] is None else result[g] + product
                held = following
            return result

        def column_sum(x):
            return jnp.sum(x, axis=0, keepdims=True)

        target = scatter_sums(
            [group_of(regrouped, g) for g in groups], [group_of(target_bound, g) for g in groups],
            early=2,
        )
        first_norms = [total(column_sum(target[g] * target[g])) for g in groups]
        lows = [t.astype(jnp.bfloat16) for t in target]
        bound_norms = lax.optimization_barrier(first_norms)
        first_norms = lax.optimization_barrier(bound_norms)
        fitted0 = gather_times(lows)
        fitted_low = [f.astype(jnp.bfloat16) for f in fitted0]
        curvature = [
            total(
                column_sum(fitted0[g] * fitted_low[g].astype(jnp.float32))
                + ridge_param * column_sum(lows[g].astype(jnp.float32) * target[g]),
            )
            for g in groups
        ]
        gain = 1.02 * subsets * float(n) ** 0.5
        image = scatter_sums(
            fitted_low, [jnp.maximum(gain * jnp.sqrt(v), 1e-30) for v in bound_norms]
        )
        alpha0 = [first_norms[g] / curvature[g] for g in groups]
        residual = [
            target[g] - alpha0[g] * (image[g] + ridge_param * target[g]) for g in groups
        ]
        residual, lows = lax.optimization_barrier(
            (residual, [r.astype(jnp.bfloat16) for r in residual])
        )
        norm1 = [total(column_sum(residual[g] * residual[g])) for g in groups]
        beta = [norm1[g] / first_norms[g] for g in groups]
        direction = [residual[g] + beta[g] * target[g] for g in groups]
        fresh = gather_times(lows)
        fitted1 = [fresh[g] + beta[g] * fitted0[g] for g in groups]
        fitted_low = [f.astype(jnp.bfloat16) for f in fitted1]
        curvature = [
            total(
                column_sum(fitted1[g] * fitted_low[g].astype(jnp.float32))
                + ridge_param * column_sum(direction[g] * direction[g]),
            )
            for g in groups
        ]
        direction_norm = [norm1[g] + beta[g] * beta[g] * first_norms[g] for g in groups]
        image = scatter_sums(
            fitted_low, [jnp.maximum(1.5 * gain * jnp.sqrt(v), 1e-30) for v in direction_norm]
        )
        alpha1 = [norm1[g] / curvature[g] for g in groups]
        weights = jnp.concatenate(
            [alpha0[g] * target[g] + alpha1[g] * direction[g] for g in groups], axis=1
        )
        residual = [
            residual[g] - alpha1[g] * (image[g] + ridge_param * direction[g]) for g in groups
        ]
        last = jnp.concatenate([column_sum(r * r) for r in residual], axis=1)
        last = total(last)
        ratio = last / jnp.concatenate(first_norms, axis=1)
        return weights, jnp.sqrt(ratio).reshape(columns)

    return per_device


def solution(mesh):
    in_specs = (P(("rows", "cols"), None), P("rows", None), P())
    out_specs = (P("rows", "cols"), P("cols"))
    body = make_body(mesh.shape["rows"], mesh.shape["cols"])

    return jax.shard_map(body, mesh=mesh, in_specs=in_specs, out_specs=out_specs, check_vma=False)
```
